32 devices in a mesh: fem: 4 (over y, x), bem: 8 (over z, core).
Axes of the slice: x: 2, y: 2, z: 4, core: 2. Of those that a mesh axis runs over, the one named last changes fastest.
Arguments:
- fem_field: float32 [32, 64, 32, 128], P('fem', 'bem'), may hold values from -6 to 6
- fem_source: float32 [32, 64, 32, 128], P('fem', 'bem'), may hold values from -6 to 6
- reaction: float32 [32, 64, 32], P('fem', 'bem'), may hold values from 0.5 to 3
- bem_density: float32 [128, 8192], P(None, 'bem'), may hold values from -6 to 6
- bem_source: float32 [128, 8192], P(None, 'bem'), may hold values from -6 to 6
- bem_diagonal: float32 [8192], P('bem'), may hold values from 2 to 6
- near_blocks: bfloat16 [16, 48, 512, 512], P('bem', 'fem'), may hold values from -0.0390625 to 0.0390625
- near_pairs: int32 [16, 48], P('bem'), may hold values from 0 to 15, as said below
- low_left: bfloat16 [16, 32, 512], P('bem'), may hold values from -1 to 1
- low_right: bfloat16 [16, 32, 512], replicated, may hold values from -0.25 to 0.25
- centers: float32 [16, 3], replicated, may hold values from 0 to 4
- trace_cell: int32 [8192], P(('fem', 'bem')), may hold values from 0 to 2047
- trace_bank: int32 [8192, 1], P(('fem', 'bem')), may hold values from 0 to 7; in each aligned block of 256 rows (0 to 255, 256 to 511, ...) at most 32 rows name the same one
- trace_row: int32 [8192], P(('fem', 'bem')), may hold values from 0 to 1023
Outputs:
- fem_out: float32 [32, 64, 32, 128], P('fem', 'bem')
- bem_out: float32 [128, 8192], P('fem', 'bem')
The draws below stay inside these ranges and needn't reach their ends.
Inputs may be any that keep to these rules, and one draw needn't show every extreme that they name: `trace_bank`: among the 256 slots of one device no bem index is named more than 32 times, and some device names some index exactly 32 times. Panel p's near-field source panels are held by bem indices within two of p's own, counted around the bem axis: near_pairs[p, k] // 2 - p // 2 is -2, -1, 0, 1 or 2 modulo 8.
All inputs are finite; a program needn't handle non-finite values.
Results may differ from the reference program's by a relative error of at most 0.0028.
Values may be sent and summed in bfloat16 or wider, within the bound.
A program may use at most 128 MiB of HBM per device.

```python
import math
import jax
import jax.numpy as jnp
import numpy as np
from jax import lax

E = 128
CX = 8
CY = 8
CZ = 32
PANEL = 512
RANK = 32
NEAR = 48
PANEL_DEV = 2
TR_DEV = 256
CAP = 32
ITERS = 3
NX = 32
NY = 64
PANELS = 16
NB = 8192
SLOTS = 8192
N_FEM = 4
N_BEM = 8


def draw_near_pairs(key, part):
    home = jnp.arange(PANELS, dtype=jnp.int32)[:, None] // PANEL_DEV
    offset_bank = jax.random.randint(jax.random.fold_in(key, 11), (PANELS, NEAR), -2, 3)
    within = jax.random.randint(jax.random.fold_in(key, 12), (PANELS, NEAR), 0, PANEL_DEV)
    return ((home + offset_bank) % N_BEM * PANEL_DEV + within).astype(jnp.int32)


def with_ends(values, own_key, low, top_value):
    shape = values.shape
    place = [jax.random.randint(jax.random.fold_in(own_key, axis), (), 0, shape[axis]) for axis in range(len(shape))]
    values = values.at[tuple(place)].set(low)
    longest = shape.index(max(shape))
    place[longest] = (place[longest] + 1) % shape[longest]
    return values.at[tuple(place)].set(top_value)


def block_levels(rng, extent, cuts, least, high):
    def one(position, blocks):
        heights = jax.random.uniform(jax.random.fold_in(jax.random.fold_in(rng, 6), position), (blocks,), jnp.float32, least / len(cuts), high / len(cuts))
        return jnp.repeat(jnp.exp(heights), extent[position] // blocks).reshape((-1,) + (1,) * (len(extent) - position - 1))

    level = one(*cuts[0])
    for cut in cuts[1:]:
        level = level * one(*cut)
    return level


def shared_out(rng, own, number, rows, count, top, reach, skew):
    ranking = jax.random.permutation(rng, count)
    packed, ordinary = load_shares(count, rows * top, reach, skew, True), load_shares(count, rows * top, reach, skew, False)
    places = jnp.arange(count)

    def named(sizes, offset_by):
        used = int((sizes > 0).sum())
        fixed = max(1, used // 4)
        passed = fixed + (places - fixed + offset_by * (used - fixed)) % max(1, count - fixed)
        return jnp.zeros((count,), jnp.int32).at[ranking[jnp.where(places < fixed, places, passed)]].set(jnp.asarray(sizes, jnp.int32))

    sizes = jnp.where(number % 4 == 0, named(packed, number // 4), named(ordinary, number - number // 4 - 1))
    mixed = jax.random.permutation(jax.random.fold_in(own, 3), count)
    giver, sink = mixed[0:count // 2 * 2:2], mixed[1:count // 2 * 2:2]
    margin = jnp.minimum(sizes[giver] - 1, reach - sizes[sink]) // 2
    margin = jnp.where((giver == ranking[0]) | (sink == ranking[0]) | (sizes[sink] == 0), 0, jnp.maximum(margin, 0))
    passed = jax.random.randint(jax.random.fold_in(own, 4), (count // 2,), 0, 1 << 20) % (margin + 1)
    sizes = sizes.at[giver].add(-passed).at[sink].add(passed)
    labels = jnp.searchsorted(jnp.cumsum(sizes), jnp.arange(rows * top), side="right").astype(jnp.int32)
    table = labels.reshape(top, rows).T
    table = table[jax.random.permutation(jax.random.fold_in(own, 1), rows)]
    offset_by = jax.random.randint(jax.random.fold_in(own, 2), (rows, 1), 0, top)
    return jnp.take_along_axis(table, (jnp.arange(top)[None, :] + offset_by) % top, axis=1)


def load_shares(count, total, most, lean, full):
    weights = [(1 << 20) // math.isqrt(standing ** lean) + 1 for standing in range(1, count + 1)]
    largest = most if full else min(most, max(-(-total // count), total * weights[0] // sum(weights)))
    least = 1 if total - largest >= count - 1 else 0
    counts, rest = [largest] + [least] * (count - 1), total - largest - least * (count - 1)
    while rest > 0:
        candidates = [i for i in range(1, count) if counts[i] < largest] or [i for i in range(1, count) if counts[i] < most]
        mass, budget = sum([weights[i] for i in candidates]), rest
        for i in candidates:
            extra = min(most - counts[i], max(1, budget * weights[i] // mass), rest)
            counts[i] = counts[i] + extra
            rest = rest - extra
    return np.array(counts)


def gaussian(own_key, shape, spread, most, shards=(), kind=jnp.bfloat16):
    drawn = spread * jax.random.normal(own_key, shape, jnp.float32)
    if shards:
        drawn = drawn * block_levels(own_key, shape, shards, -0.22, 0.18)
    return jnp.clip(drawn, -most, most).astype(kind)


def setup_inputs(seed: int = 0) -> dict:
    seeds = jax.random.split(jax.random.key(seed), 15)
    fem_field = gaussian(seeds[0], (NX, NY, CZ, E), 1.0, 6.0, ((0, 4), (1, 8)), jnp.float32)
    fem_source = gaussian(seeds[1], (NX, NY, CZ, E), 1.0, 6.0, ((0, 4), (1, 8)), jnp.float32)
    reaction = jnp.clip(0.5 + 2.5 * jax.random.uniform(seeds[2], (NX, NY, CZ), jnp.float32) ** block_levels(seeds[2], (NX, NY, CZ), ((0, 4), (1, 8)), -0.2, 0.2), 0.5, 3.0)
    bem_density = gaussian(seeds[3], (E, NB), 1.0, 6.0, ((1, 8),), jnp.float32)
    bem_source = gaussian(seeds[4], (E, NB), 1.0, 6.0, ((1, 8),), jnp.float32)
    bem_diagonal = jnp.clip(jnp.exp(math.log(6.0) - 1.0986123 * jax.random.uniform(seeds[5], (NB,), jnp.float32) ** block_levels(seeds[5], (NB,), ((0, 8),), -0.2, 0.2)), 2.0, 6.0)
    near_blocks = gaussian(seeds[6], (PANELS, NEAR, PANEL, PANEL), (NEAR * PANEL) ** -0.5, 0.0390625, ((0, 8), (1, 4)))
    near_pairs = draw_near_pairs(jax.random.fold_in(seeds[14], 71), 0)
    low_left = gaussian(seeds[8], (PANELS, RANK, PANEL), RANK ** -0.5, 1.0, ((0, 8),))
    low_right = gaussian(seeds[9], (PANELS, RANK, PANEL), PANEL ** -0.5, 0.25)
    centers = jnp.clip(jax.random.uniform(seeds[10], (PANELS, 3), jnp.float32, 0.0, 4.0), 0.0, 4.0)
    trace_cell = with_ends(jax.random.randint(seeds[11], (SLOTS,), 0, CX * CY * CZ), jax.random.fold_in(seeds[11], 1), 0, (CX * CY * CZ) - 1).astype(jnp.int32)
    trace_bank_keys = jax.random.split(jax.random.fold_in(seeds[12], 1), SLOTS // TR_DEV)
    trace_bank_turns = jax.random.permutation(jax.random.fold_in(seeds[12], 3), SLOTS // TR_DEV)
    trace_bank = jax.vmap(lambda own, number: shared_out(jax.random.fold_in(seeds[12], 2), own, number, TR_DEV, N_BEM, 1, CAP, 2))(trace_bank_keys, trace_bank_turns).reshape((SLOTS, 1))
    trace_row = with_ends(jax.random.randint(seeds[13], (SLOTS,), 0, PANEL_DEV * PANEL), jax.random.fold_in(seeds[13], 1), 0, (PANEL_DEV * PANEL) - 1).astype(jnp.int32)
    return dict(fem_field=fem_field, fem_source=fem_source, reaction=reaction, bem_density=bem_density, bem_source=bem_source, bem_diagonal=bem_diagonal, near_blocks=near_blocks, near_pairs=near_pairs, low_left=low_left, low_right=low_right, centers=centers, trace_cell=trace_cell, trace_bank=trace_bank, trace_row=trace_row)


HIGHEST = lax.Precision.HIGHEST


def stiffness(state, reaction):
    padded = jnp.pad(state, ((1, 1), (1, 1), (1, 1), (0, 0)))
    beside = padded[2:, 1:-1, 1:-1] + padded[:-2, 1:-1, 1:-1]
    beside = beside + padded[1:-1, 2:, 1:-1] + padded[1:-1, :-2, 1:-1]
    beside = beside + padded[1:-1, 1:-1, 2:] + padded[1:-1, 1:-1, :-2]
    return (6.0 + reaction)[..., None] * state - beside


def by_device(state):
    blocks = state.reshape(N_FEM, CX, N_BEM, CY, CZ, E).transpose(0, 2, 1, 3, 4, 5)
    return blocks.reshape(N_FEM * N_BEM * CX * CY * CZ, E)


def from_device(flat):
    blocks = flat.reshape(N_FEM, N_BEM, CX, CY, CZ, E).transpose(0, 2, 1, 3, 4, 5)
    return blocks.reshape(N_FEM * CX, N_BEM * CY, CZ, E)


def near_field(rounded, near_blocks, near_pairs):
    grouped = rounded.reshape(E, PANELS, PANEL)

    def one_panel(pieces):
        blocks, pairs = pieces
        chosen = jnp.take(grouped, pairs, axis=1).astype(jnp.float32)
        return jnp.einsum("ekn,knm->em", chosen, blocks.astype(jnp.float32), precision=HIGHEST)

    rows = lax.map(one_panel, (near_blocks, near_pairs))
    return rows.transpose(1, 0, 2).reshape(E, PANELS * PANEL)


def far_field(rounded, low_left, low_right, centers, near_pairs):
    grouped = rounded.reshape(E, PANELS, PANEL).astype(jnp.float32)
    reduced = jnp.einsum("eqn,qrn->eqr", grouped, low_right.astype(jnp.float32), precision=HIGHEST).astype(jnp.bfloat16)
    reduced = lax.optimization_barrier(reduced).astype(jnp.float32)
    offsets = centers[:, None, :] - centers[None, :, :]
    kernel = 1.0 / (1.0 + jnp.sum(offsets * offsets, axis=-1))
    panel_ids = jnp.arange(PANELS, dtype=jnp.int32)
    listed = jnp.any(near_pairs[:, :, None] == panel_ids[None, None, :], axis=1)
    listed = listed | (panel_ids[:, None] == panel_ids[None, :])
    kernel = jnp.where(listed, 0.0, kernel)
    weights = jnp.einsum("pq,eqr->epr", kernel, reduced, precision=HIGHEST)
    distant = jnp.einsum("epr,prn->epn", weights, low_left.astype(jnp.float32), precision=HIGHEST)
    return distant.reshape(E, PANELS * PANEL)


def reference(fem_field, fem_source, reaction, bem_density, bem_source, bem_diagonal, near_blocks, near_pairs, low_left, low_right, centers, trace_cell, trace_bank, trace_row):
    slot_device = jnp.arange(trace_cell.shape[0], dtype=jnp.int32) // TR_DEV
    cell_index = (slot_device * (CX * CY * CZ) + trace_cell).astype(jnp.int32)
    node_index = (trace_bank[:, 0] * (PANEL_DEV * PANEL) + trace_row).astype(jnp.int32)
    fem_state = fem_field
    density = bem_density
    for sweep in range(ITERS):
        rounded = lax.optimization_barrier(density.astype(jnp.bfloat16))
        flat_fem = by_device(fem_state)
        traced = jnp.zeros((PANELS * PANEL, E), jnp.float32).at[node_index].add(flat_fem[cell_index])
        applied = near_field(rounded, near_blocks, near_pairs) + far_field(rounded, low_left, low_right, centers, near_pairs) + traced.T
        coupled_flat = jnp.zeros((N_FEM * N_BEM * CX * CY * CZ, E), jnp.float32).at[cell_index].add(density.T[node_index])
        coupled = from_device(coupled_flat)
        fem_next = fem_state + (fem_source - stiffness(fem_state, reaction) - coupled) / (6.0 + reaction)[..., None]
        density = density + (bem_source - applied) / bem_diagonal[None, :]
        fem_state = fem_next
    return fem_state, density
```

```python
import functools

import jax
import jax.numpy as jnp
from jax import lax
from jax.experimental import pallas as pl
from jax.experimental.pallas import tpu as pltpu
from jax.sharding import PartitionSpec as P

CAP = 32
ITERS = 3
REACH = 2
F32 = jnp.float32
BF16 = jnp.bfloat16
MESH = pl.DeviceIdType.MESH


def dot(a, b, ca=1, cb=0):
    return lax.dot_general(a, b, (((ca,), (cb,)), ((), ())), preferred_element_type=F32)


def hot(test):
    return jnp.where(test, 1.0, 0.0).astype(BF16)


def layout(d):
    f, b, share, pd, rows = d.f, d.b, d.share, d.pd, d.rows
    exc, dest = d.exc, d.dest
    spots = (2 * REACH + 1) * pd

    def one(kind, *shape):
        return pltpu.VMEM(shape, kind)

    def each(kind, *shape):
        return [one(kind, *shape) for _ in range(ITERS)]

    return dict(
        x=each(BF16, spots, exc, rows),
        psend=each(BF16, pd, exc, rows),
        precv=each(BF16, pd, f - 1, share, rows),
        xface_send=each(BF16, 2, d.cy, d.cz, exc),
        yface_send=each(BF16, 2, d.cx, d.cz, exc),
        xface_recv=each(BF16, 2, d.cy, d.cz, exc),
        yface_recv=each(BF16, 2, d.cx, d.cz, exc),
        out_send=each(BF16, b, CAP, exc),
        out_recv=each(BF16, b, CAP, exc),
        val_send=each(BF16, b, CAP, exc),
        val_recv=each(BF16, b, CAP, exc),
        red_send=each(BF16, share, 128),
        red_recv=each(BF16, b, share, 128),
        fem=[one(F32, d.cx + 2, d.cy + 2, d.cz, exc) for _ in range(2)],
        acc=one(F32, pd, exc, rows),
        den=one(F32, pd, share, rows),
        row_send=one(F32, b, CAP, 128),
        row_recv=one(F32, b, CAP, 128),
        load=one(F32, d.cx, d.cy, d.cz, exc),
        inv=one(F32, d.cx, d.cy, d.cz, exc),
        whole=one(F32, exc, pd * rows),
        bsrc=one(F32, share, pd * rows),
        blocks=one(BF16, pd, d.group, rows, rows),
        pick_cell=one(BF16, d.cx, dest, d.cy * d.cz),
        put_cell=one(BF16, d.cx, d.cy * d.cz, dest),
        pick_row=one(BF16, dest, pd * rows),
        right=one(BF16, pd, d.rank, rows),
        right_wide=one(BF16, pd, 128, rows),
        left_wide=one(BF16, pd, 128, rows),
        traced=one(F32, exc, pd * rows),
        base=one(F32, share, pd * rows),
        bank=one(jnp.int32, 1, d.slots),
        node=one(jnp.int32, 1, d.slots),
        cell=one(jnp.int32, 1, d.slots),
        pairs=one(jnp.int32, pd, d.pairs),
        centers=one(F32, 3, b * pd),
        reaction=one(F32, d.cx, d.cy, d.cz),
        diag=one(F32, 1, pd * rows),
        left=one(BF16, pd, d.rank, rows),
        kernel=one(F32, pd, b * pd, 128),
    )


def solve_kernel(
    d,
    pairs_ref,
    bank_hbm,
    node_hbm,
    cell_hbm,
    pairs_hbm,
    centers_hbm,
    reaction_hbm,
    diag_hbm,
    left_hbm,
    fem_hbm,
    load_hbm,
    density_hbm,
    bsrc_hbm,
    blocks_hbm,
    right_hbm,
    fem_out,
    bem_out,
    *scratch,
):
    places = jax.tree.structure(layout(d))
    r = Dims(**jax.tree.unflatten(places, scratch[:-3]))
    send_sem, recv_sem, load_sem = scratch[-3:]
    F, B, pd, share, rows, exc = d.f, d.b, d.pd, d.share, d.rows, d.exc
    f, b = lax.axis_index("fem"), lax.axis_index("bem")
    odd = lax.rem(b, 2)
    home = REACH * pd
    arrivals, loads = iter(range(recv_sem.shape[0])), iter(range(load_sem.shape[0]))
    senders, leaving = {}, {}

    def sender(key):
        if key in leaving:
            leaving.pop(key)()
        slot = senders.setdefault(key, len(senders))
        assert slot < send_sem.shape[0]
        return send_sem.at[slot]

    def fem_peer(step):
        return (lax.rem(f + step + F, F), b)

    def flipped(flips):
        index = 0
        for i in range((F - 1).bit_length()):
            bit = lax.rem(f // (1 << i), 2)
            index += (1 - bit if flips >> i & 1 else bit) * (1 << i)
        return index

    def across_fem(flips):
        return (flipped(flips), b)

    def bem_peer(step):
        return (f, lax.rem(b + step + B, B))

    def remote(src, dst, place, ssem, rsem):
        return pltpu.make_async_remote_copy(
            src_ref=src,
            dst_ref=dst,
            send_sem=ssem,
            recv_sem=rsem,
            device_id=place,
            device_id_type=MESH,
        )

    def send(src, dst, place, key):
        copy = remote(src, dst, place, sender(key), recv_sem.at[next(arrivals)])
        copy.start()
        leaving[key] = copy.wait_send
        return copy.wait_recv

    def send_fem(src_of, dst_of, flips, size_ref, key):
        ssem, rsem = sender(key), recv_sem.at[next(arrivals)]
        for k in flips:
            remote(src_of(k), dst_of(k), across_fem(k), ssem, rsem).start()
        leaving[key] = pltpu.make_async_copy(size_ref, size_ref, ssem).wait
        return pltpu.make_async_copy(size_ref, size_ref, rsem).wait

    def fetch(src, dst):
        copy = pltpu.make_async_copy(src, dst, load_sem.at[next(loads)])
        copy.start()
        return copy

    opposite = F - 1
    nearby = range(1, F - 1)

    def spread(src_of, dst_ref, sign, key):
        ssem, rsem = sender(key), recv_sem.at[next(arrivals)]
        for s in range(1, B):
            remote(src_of(s), dst_ref.at[s], bem_peer(sign * s), ssem, rsem).start()
        rest = dst_ref.at[1:]
        leaving[key] = pltpu.make_async_copy(rest, rest, ssem).wait
        return pltpu.make_async_copy(rest, rest, rsem).wait

    whole_in = fetch(density_hbm, r.whole)
    small_in = [
        fetch(bank_hbm, r.bank),
        fetch(node_hbm, r.node),
        fetch(cell_hbm, r.cell),
    ]
    first = fetch(fem_hbm, r.fem[0].at[1 : d.cx + 1, 1 : d.cy + 1])
    right_in = fetch(right_hbm.at[pl.ds(b * pd, pd)], r.right)
    bsrc_in = fetch(bsrc_hbm.at[pl.ds(pl.multiple_of(f * share, share), share)], r.bsrc)
    load_in = fetch(load_hbm, r.load)
    other_in = [
        fetch(pairs_hbm, r.pairs),
        fetch(centers_hbm, r.centers),
        fetch(reaction_hbm, r.reaction),
        fetch(diag_hbm, r.diag),
        fetch(left_hbm, r.left),
        bsrc_in,
        load_in,
    ]

    barrier = pltpu.get_barrier_semaphore()
    for s in range(1, F):
        pl.semaphore_signal(barrier, inc=1, device_id=fem_peer(s), device_id_type=MESH)
    for s in range(1, B):
        pl.semaphore_signal(barrier, inc=1, device_id=bem_peer(s), device_id_type=MESH)
    blocks_in = [fetch(blocks_hbm.at[p], r.blocks.at[p]) for p in range(pd)]

    whole_in.wait()
    for p in range(pd):
        cols = slice(p * rows, (p + 1) * rows)
        r.x[0][home + p] = r.whole[:, cols].astype(BF16)
        r.den[p] = r.whole[pl.ds(pl.multiple_of(f * share, share), share), cols]
    pl.semaphore_wait(barrier, F - 1 + B - 1)

    def rows_of(index):
        return pl.ds(pl.multiple_of(index * share, share), share)

    own_rows, opposite_rows = rows_of(f), rows_of(flipped(opposite))
    state = Dims(
        faces={},
        fwd={},
        homes={},
        out={},
        own={},
        turned={},
        parts={},
        red={},
        sides={},
        val={},
        z={},
    )

    def partner_copy(n, p, which):
        x = r.x[n]
        if which == "home":
            there = jnp.where(odd == 0, -1, 1)
            source = home + p
        else:
            there = jnp.where(odd == 0, 1, -1)
            source = (REACH + 2 * there) * pd + p
        target = (REACH + there) * pd + p
        place = (f, b + 1 - 2 * odd)
        return send(x.at[pl.ds(source, 1)], x.at[pl.ds(target, 1)], place, (which, p))

    def along_bem(n, p, span, key):
        x = r.x[n]
        return {
            side: send(
                x.at[home + p, span],
                x.at[(REACH - side) * pd + p, span],
                bem_peer(side),
                (key, p, side),
            )
            for side in (2, -2)
        }

    def start_share(n, p):
        mine = r.x[n].at[home + p, own_rows]
        state.z[n, p] = along_bem(n, p, own_rows, "z")
        if n > 0:
            size = r.precv[n].at[p]
            state.own[n, p] = [
                send_fem(
                    lambda k: mine, lambda k: mine, flips, size.at[0 : len(flips)], (tag, p)
                )
                for tag, flips in (("far", (opposite,)), ("own", nearby))
            ]

    def turn(n, p):
        if n > 0:
            state.own[n, p][0]()
        state.turned[n, p] = along_bem(n, p, opposite_rows, "m")

    def forward(n, p):
        state.fwd[n, p] = []
        for side in (2, -2):
            state.z[n, p][side]()
            piece = r.x[n].at[(REACH - side) * pd + p, own_rows]
            size = r.precv[n].at[p, 0 : len(nearby)]
            state.fwd[n, p].append(
                send_fem(
                    lambda k: piece, lambda k: piece, nearby, size, ("fwd", p, side)
                )
            )

    def homes(n, p):
        if n > 0:
            state.own[n, p][1]()
        state.homes[n, p] = partner_copy(n, p, "home")

    def sides(n, p):
        for arrive in (*state.turned[n, p].values(), *state.fwd[n, p]):
            arrive()
        state.sides[n, p] = partner_copy(n, p, "sides")

    def reduce_own(n):
        total = 0.0
        for p in range(pd):
            mine = r.x[n][home + p, own_rows, :]
            total += dot(mine, r.right_wide[p], 1, 1)
        r.red_send[n][...] = total.astype(BF16)
        r.red_recv[n][0] = total.astype(BF16)
        state.red[n] = spread(lambda s: r.red_send[n], r.red_recv[n], 1, "red")

    def send_picked(n, acc):
        out = acc.astype(BF16).reshape(B, CAP, exc)
        r.out_send[n][...] = out
        r.out_recv[n][0] = out[0]
        state.out[n] = spread(lambda s: r.out_send[n].at[s], r.out_recv[n], 1, "out")

    def send_faces(n):
        fem = r.fem[n % 2]
        xs, ys = r.xface_send[n], r.yface_send[n]
        xr, yr = r.xface_recv[n], r.yface_recv[n]
        xs[0] = fem[d.cx, 1 : d.cy + 1].astype(BF16)
        xs[1] = fem[1, 1 : d.cy + 1].astype(BF16)
        ys[0] = fem[1 : d.cx + 1, d.cy].astype(BF16)
        ys[1] = fem[1 : d.cx + 1, 1].astype(BF16)
        waits = []
        for out, got, rank, size, peer in ((xs, xr, f, F, fem_peer), (ys, yr, b, B, bem_peer)):
            for i, step in enumerate((1, -1)):
                goes = rank < size - 1 if step == 1 else rank > 0
                comes = rank > 0 if step == 1 else rank < size - 1
                key = ("face", len(waits))
                copy = remote(out.at[i], got.at[i], peer(step), sender(key), recv_sem.at[next(arrivals)])
                pl.when(goes)(copy.start)
                leaving[key] = functools.partial(pl.when(goes), copy.wait_send)
                waits.append((comes, copy))
        state.faces[n] = waits

    def take_faces(n):
        fem = r.fem[n % 2]
        xr, yr = r.xface_recv[n], r.yface_recv[n]

        def put(i):
            if i == 0:
                fem[0, 1 : d.cy + 1] = xr[0].astype(F32)
            elif i == 1:
                fem[d.cx + 1, 1 : d.cy + 1] = xr[1].astype(F32)
            elif i == 2:
                fem[1 : d.cx + 1, 0] = yr[0].astype(F32)
            else:
                fem[1 : d.cx + 1, d.cy + 1] = yr[1].astype(F32)

        def clear(i):
            if i < 2:
                fem[(0, d.cx + 1)[i], 1 : d.cy + 1] = jnp.zeros((d.cy, d.cz, exc), F32)
            else:
                fem[1 : d.cx + 1, (0, d.cy + 1)[i - 2]] = jnp.zeros((d.cx, d.cz, exc), F32)

        for i, (comes, copy) in enumerate(state.faces[n]):

            def take(i=i, copy=copy):
                copy.wait_recv()
                put(i)

            pl.when(comes)(take)
            pl.when(jnp.logical_not(comes))(functools.partial(clear, i))

    def picked_first():
        def body(x, acc):
            plane = r.fem[0][x + 1, 1 : d.cy + 1].astype(BF16).reshape(d.cy * d.cz, exc)
            return acc + dot(r.pick_cell[x], plane)

        return lax.fori_loop(0, d.cx, body, jnp.zeros((d.dest, exc), F32))

    def fem_step(n):
        take_faces(n)
        state.val[n]()
        last = n == ITERS - 1
        old, fresh = r.fem[n % 2], r.fem[(n + 1) % 2]
        values = r.val_recv[n][...].reshape(d.dest, exc)
        level = lax.broadcasted_iota(jnp.int32, (d.cy, d.cz, exc), 1)

        def body(x, acc):
            coupled = dot(r.put_cell[x], values).reshape(d.cy, d.cz, exc)
            here = old[x + 1, 1 : d.cy + 1]
            beside = old[x, 1 : d.cy + 1] + old[x + 2, 1 : d.cy + 1]
            beside += old[x + 1, 0 : d.cy] + old[x + 1, 2 : d.cy + 2]
            beside += jnp.where(level > 0, pltpu.roll(here, 1, 1), 0.0)
            beside += jnp.where(level < d.cz - 1, pltpu.roll(here, d.cz - 1, 1), 0.0)
            result = (r.load[x] + beside - coupled) * r.inv[x]
            if last:
                fem_out[x] = result
                return acc
            fresh[x + 1, 1 : d.cy + 1] = result
            plane = result.astype(BF16).reshape(d.cy * d.cz, exc)
            return acc + dot(r.pick_cell[x], plane)

        acc = lax.fori_loop(0, d.cx, body, jnp.zeros((8 if last else d.dest, exc), F32))
        if not last:
            send_picked(n + 1, acc)

    def trace_values(n):
        values = 0.0
        for p in range(pd):
            values += dot(r.pick_row[:, p * rows : (p + 1) * rows], r.x[n][home + p], 1, 1)
        out = values.astype(BF16).reshape(B, CAP, exc)
        r.val_send[n][...] = out
        r.val_recv[n][0] = out[0]
        state.val[n] = spread(lambda s: r.val_send[n].at[s], r.val_recv[n], -1, "val")

    def trace_fem(n):
        state.out[n]()
        incoming = r.out_recv[n][...].reshape(d.dest, exc)
        r.traced[...] = dot(incoming, r.pick_row[...], 0, 0)

    def far(n):
        state.red[n]()
        for p in range(pd):
            total = jnp.zeros((share, 128), F32)
            for s in range(B):
                scale = jnp.zeros((1, 128), F32)
                for q in range(pd):
                    at = lax.rem(b - s + B, B) * pd + q
                    group = (lane128 >= q * d.rank) & (lane128 < (q + 1) * d.rank)
                    scale = jnp.where(group, r.kernel[p, pl.ds(at, 1), :], scale)
                total += r.red_recv[n][s].astype(F32) * scale
            high = total.astype(BF16)
            low = (total - high.astype(F32)).astype(BF16)
            distant = dot(high, r.left_wide[p]) + dot(low, r.left_wide[p])
            cols = slice(p * rows, (p + 1) * rows)
            r.base[:, cols] = r.bsrc[:, cols] - distant

    def near(n):
        for p in range(pd):
            state.sides[n, p]()
            state.homes[n, p]()
        x = r.x[n]
        for p in range(pd):
            cols = slice(p * rows, (p + 1) * rows)
            acc = r.traced[:, cols]
            for k in range(d.group):
                pair = pairs_ref[p, f * d.group + k]
                spot = lax.rem(pair - b * pd + REACH * pd + B * pd, B * pd)
                spot = jnp.minimum(spot, (2 * REACH + 1) * pd - 1)
                acc += dot(x[spot], r.blocks[p, k])
            r.acc[p] = acc
            out, got = r.psend[n], r.precv[n]
            out[p] = acc.astype(BF16)
            state.parts[n, p] = send_fem(
                lambda k: out.at[p, rows_of(flipped(k))],
                lambda k: got.at[p, k - 1],
                range(F - 1, 0, -1),
                got.at[p],
                ("part", p),
            )

    def update(n, p):
        state.parts[n, p]()
        last = n == ITERS - 1
        cols = slice(p * rows, (p + 1) * rows)
        total = r.acc[p, own_rows, :]
        for k in range(F - 1):
            total += r.precv[n][p, k].astype(F32)
        fresh = r.den[p] + (r.base[:, cols] - total) / r.diag[:, cols]
        if last:
            bem_out[:, cols] = fresh
        else:
            r.den[p] = fresh
            r.x[n + 1][home + p, own_rows, :] = fresh.astype(BF16)
            start_share(n + 1, p)

    for p in range(pd):
        start_share(0, p)
    for p in range(pd):
        turn(0, p)
        homes(0, p)

    def column(row):
        size = row.shape[1]
        down = lax.broadcasted_iota(jnp.int32, (size, size), 0)
        across = lax.broadcasted_iota(jnp.int32, (size, size), 1)
        return jnp.sum(jnp.where(down == across, row, 0.0), axis=1, keepdims=True)

    count, dest = d.slots, d.dest
    lane128 = lax.broadcasted_iota(jnp.int32, (1, 128), 1)
    for copy in small_in:
        copy.wait()
    node_row = r.node[...].astype(F32)
    cell_row = r.cell[...].astype(F32)
    step_row = lax.rem(r.bank[...] - b + B, B).astype(F32)
    down = lax.broadcasted_iota(jnp.int32, (count, count), 0)
    across = lax.broadcasted_iota(jnp.int32, (count, count), 1)
    earlier = (column(step_row) == step_row) & (down < across)
    order = jnp.sum(jnp.where(earlier, 1.0, 0.0), axis=0, keepdims=True)
    target = step_row * CAP + order
    lands = lax.broadcasted_iota(jnp.int32, (dest, count), 0).astype(F32) == target
    row_col = jnp.sum(jnp.where(lands, node_row + 1.0, 0.0), axis=1, keepdims=True) - 1.0
    cell_col = jnp.sum(jnp.where(lands, cell_row + 1.0, 0.0), axis=1, keepdims=True) - 1.0
    row_wide = jnp.broadcast_to(row_col, (dest, 128)).reshape(B, CAP, 128)
    r.row_send[...] = row_wide
    r.row_recv[0] = row_wide[0]
    row_in = spread(lambda s: r.row_send.at[s], r.row_recv, 1, "row")

    right_in.wait()
    for p in range(pd):
        r.right_wide[p] = jnp.zeros((128, rows), BF16)
        r.right_wide[p, p * d.rank : (p + 1) * d.rank, :] = r.right[p]
    reduce_own(0)

    plane = d.cy * d.cz
    ids_lane = lax.broadcasted_iota(jnp.int32, (dest, plane), 1).astype(F32)
    for x in range(d.cx):
        r.pick_cell[x] = hot(cell_col - float(x * plane) == ids_lane)
    first.wait()
    send_picked(0, picked_first())
    for p in range(pd):
        forward(0, p)
    send_faces(0)

    lands_t = lax.broadcasted_iota(jnp.int32, (count, dest), 1).astype(F32) == column(target)
    cell_send = (
        jnp.sum(jnp.where(lands_t, column(cell_row) + 1.0, 0.0), axis=0, keepdims=True) - 1.0
    )
    ids_down = lax.broadcasted_iota(jnp.int32, (plane, dest), 0).astype(F32)
    for x in range(d.cx):
        r.put_cell[x] = hot(cell_send - float(x * plane) == ids_down)

    for copy in other_in:
        copy.wait()
    for p in range(pd):
        r.left_wide[p] = jnp.zeros((128, rows), BF16)
        for q in range(pd):
            r.left_wide[p, q * d.rank : (q + 1) * d.rank, :] = r.left[p]
    total = B * pd
    panel_row = lax.broadcasted_iota(jnp.int32, (1, total), 1)
    panel_col = lax.broadcasted_iota(jnp.int32, (total, 1), 0)
    for p in range(pd):
        own = b * pd + p
        square = jnp.zeros((total, 1), F32)
        for i in range(3):
            place = r.centers[i : i + 1, :]
            mine = jnp.sum(jnp.where(panel_row == own, place, 0.0), axis=1, keepdims=True)
            apart = mine - column(place)
            square += apart * apart
        named = jnp.where(r.pairs[p : p + 1, :] == panel_col, 1.0, 0.0)
        listed = jnp.max(named, axis=1, keepdims=True) + jnp.where(panel_col == own, 1.0, 0.0)
        weight = jnp.where(listed > 0.0, 0.0, 1.0 / (1.0 + square))
        r.kernel[p] = jnp.broadcast_to(weight, (total, 128))

    def spread_inverse(x, carry):
        inverse = 1.0 / (6.0 + r.reaction[x])
        for y in range(d.cy):
            wide = jnp.broadcast_to(column(inverse[y : y + 1, :]), (d.cz, exc))
            r.inv[x, y] = wide
        return carry

    lax.fori_loop(0, d.cx, spread_inverse, 0)

    for n in range(ITERS):
        last = n == ITERS - 1
        if n > 0:
            reduce_own(n)
            fem_step(n - 1)
            for p in range(pd):
                turn(n, p)
                forward(n, p)
            send_faces(n)
            for p in range(pd):
                homes(n, p)
        if n == 0:
            row_in()
            wanted = r.row_recv[...].reshape(dest, 128)
            lanes = lax.broadcasted_iota(jnp.int32, (dest, 128), 1).astype(F32)
            for j in range(pd * rows // 128):
                r.pick_row[:, j * 128 : (j + 1) * 128] = hot(wanted - float(j * 128) == lanes)
        trace_values(n)
        trace_fem(n)
        far(n)
        if n == 0:
            for copy in blocks_in:
                copy.wait()
        for p in range(pd):
            sides(n, p)
        near(n)
        if last:
            fem_step(n)
        for p in range(pd):
            update(n, p)

    for finish in leaving.values():
        finish()


def hand_over(fem_in, bem_in, fem_out, bem_out, out_sem):
    moves = ((fem_in, fem_out), (bem_in, bem_out))
    outs = [pltpu.make_async_copy(m, o, out_sem.at[i]) for i, (m, o) in enumerate(moves)]
    for copy in outs:
        copy.start()
    for copy in outs:
        copy.wait()


class Dims:
    def __init__(self, **items):
        self.__dict__.update(items)


def shards(
    fem_field,
    fem_source,
    reaction,
    bem_density,
    bem_source,
    bem_diagonal,
    near_blocks,
    near_pairs,
    low_left,
    low_right,
    centers,
    trace_cell,
    trace_bank,
    trace_row,
):
    d = Dims()
    d.f, d.b = lax.axis_size("fem"), lax.axis_size("bem")
    d.pd, d.group, d.rows, _ = near_blocks.shape
    d.rank = low_right.shape[1]
    d.cx, d.cy, d.cz, d.exc = fem_field.shape
    d.share = d.exc // d.f
    d.slots = trace_cell.shape[0]
    d.dest = d.b * CAP
    d.pairs = near_pairs.shape[1]

    items = jax.tree.leaves(layout(d))
    vmem = pl.BlockSpec(memory_space=pltpu.VMEM)
    far_off = pl.BlockSpec(memory_space=pltpu.HBM)
    results = pl.pallas_call(
        functools.partial(solve_kernel, d),
        out_shape=[
            pltpu.VMEM(fem_field.shape, F32),
            pltpu.VMEM((d.share, d.pd * d.rows), F32),
        ],
        in_specs=[pl.BlockSpec(memory_space=pltpu.SMEM)] + [far_off] * 14,
        out_specs=[vmem, vmem],
        scratch_shapes=items
        + [
            pltpu.SemaphoreType.DMA((30,)),
            pltpu.SemaphoreType.DMA((84,)),
            pltpu.SemaphoreType.DMA((17,)),
        ],
        cost_estimate=pl.CostEstimate(flops=1 << 33, bytes_accessed=1 << 24, transcendentals=0),
        compiler_params=pltpu.CompilerParams(
            collective_id=0, has_side_effects=True, vmem_limit_bytes=54 << 20
        ),
        name="sweeps",
    )(
        near_pairs,
        trace_bank.reshape(1, d.slots),
        trace_row[None, :],
        trace_cell[None, :],
        near_pairs,
        centers.T,
        reaction,
        bem_diagonal[None, :],
        low_left,
        fem_field,
        fem_source,
        bem_density,
        bem_source,
        near_blocks,
        low_right,
    )
    return pl.pallas_call(
        hand_over,
        out_shape=[jax.ShapeDtypeStruct(x.shape, x.dtype) for x in results],
        in_specs=[vmem] * 2,
        out_specs=[far_off] * 2,
        scratch_shapes=[pltpu.SemaphoreType.DMA((2,))],
        compiler_params=pltpu.CompilerParams(vmem_limit_bytes=4 << 20),
        name="hand_over",
    )(*results)


def solution(mesh):
    return jax.shard_map(
        shards,
        mesh=mesh,
        in_specs=(
            P("fem", "bem", None, None),
            P("fem", "bem", None, None),
            P("fem", "bem", None),
            P(None, "bem"),
            P(None, "bem"),
            P("bem"),
            P("bem", "fem", None, None),
            P("bem", None),
            P("bem", None, None),
            P(),
            P(),
            P(("fem", "bem")),
            P(("fem", "bem"), None),
            P(("fem", "bem")),
        ),
        out_specs=(P("fem", "bem", None, None), P("fem", "bem")),
        check_vma=False,
    )
```

```python
import functools

import jax
import jax.numpy as jnp
from jax import lax
from jax.experimental import pallas as pl
from jax.experimental.pallas import tpu as pltpu
from jax.sharding import PartitionSpec as P

CAP = 32
ITERS = 3
REACH = 2
F32 = jnp.float32
BF16 = jnp.bfloat16
MESH = pl.DeviceIdType.MESH


def dot(a, b, ca=1, cb=0):
    return lax.dot_general(a, b, (((ca,), (cb,)), ((), ())), preferred_element_type=F32)


def hot(test):
    return jnp.where(test, 1.0, 0.0).astype(BF16)


def layout(d):
    f, b, share, pd, rows = d.f, d.b, d.share, d.pd, d.rows
    exc, dest = d.exc, d.dest
    spots = (2 * REACH + 1) * pd

    def one(kind, *shape):
        return pltpu.VMEM(shape, kind)

    def each(kind, *shape):
        return [one(kind, *shape) for _ in range(ITERS)]

    return dict(
        x=each(BF16, spots, exc, rows),
        psend=each(BF16, pd, exc, rows),
        precv=each(BF16, pd, f - 1, share, rows),
        xface_send=each(BF16, 2, d.cy, d.cz, exc),
        yface_send=each(BF16, 2, d.cx, d.cz, exc),
        xface_recv=each(BF16, 2, d.cy, d.cz, exc),
        yface_recv=each(BF16, 2, d.cx, d.cz, exc),
        out_send=each(BF16, b, CAP, exc),
        out_recv=each(BF16, b, CAP, exc),
        val_send=each(BF16, b, CAP, exc),
        val_recv=each(BF16, b, CAP, exc),
        red_send=each(BF16, share // 2, 128),
        red_recv=each(BF16, b, share // 2, 128),
        fem=[one(F32, d.cx + 2, d.cy + 2, d.cz, exc) for _ in range(2)],
        acc=one(F32, pd, exc, rows),
        den=one(F32, pd, share, rows),
        row_send=one(F32, 1, dest),
        row_recv=one(F32, b, 1, dest),
        load=one(F32, d.cx, d.cy, d.cz, exc),
        inv=one(F32, d.cx, d.cy, d.cz, exc),
        whole=one(F32, exc, pd * rows),
        bsrc=one(F32, share, pd * rows),
        blocks=one(BF16, pd, d.group, rows, rows),
        pick_cell=one(BF16, d.cx, dest, d.cy * d.cz),
        put_cell=one(BF16, d.cx, d.cy * d.cz, dest),
        pick_row=one(BF16, dest, pd * rows),
        right=one(BF16, pd, d.rank, rows),
        right_wide=one(BF16, pd, 128, rows),
        left_wide=one(BF16, pd, 128, rows),
        traced=one(F32, exc, pd * rows),
        base=one(F32, share, pd * rows),
        bank=one(jnp.int32, 1, d.slots),
        node=one(jnp.int32, 1, d.slots),
        cell=one(jnp.int32, 1, d.slots),
        pairs=one(jnp.int32, pd, d.pairs),
        centers=one(F32, 3, b * pd),
        reaction=one(F32, d.cx, d.cy, d.cz),
        diag=one(F32, 1, pd * rows),
        left=one(BF16, pd, d.rank, rows),
        kernel=one(F32, pd, b * pd, 128),
    )


def solve_kernel(
    d,
    pairs_ref,
    bank_hbm,
    node_hbm,
    cell_hbm,
    pairs_hbm,
    centers_hbm,
    reaction_hbm,
    diag_hbm,
    left_hbm,
    fem_hbm,
    load_hbm,
    density_hbm,
    bsrc_hbm,
    blocks_hbm,
    right_hbm,
    fem_out,
    bem_out,
    *scratch,
):
    places = jax.tree.structure(layout(d))
    r = Dims(**jax.tree.unflatten(places, scratch[:-3]))
    send_sem, recv_sem, load_sem = scratch[-3:]
    F, B, pd, share, rows, exc = d.f, d.b, d.pd, d.share, d.rows, d.exc
    f, b = lax.axis_index("fem"), lax.axis_index("bem")
    odd = lax.rem(b, 2)
    home = REACH * pd
    arrivals, loads = iter(range(recv_sem.shape[0])), iter(range(load_sem.shape[0]))
    senders, leaving = {}, {}

    def sender(key):
        if key in leaving:
            leaving.pop(key)()
        slot = senders.setdefault(key, len(senders))
        assert slot < send_sem.shape[0]
        return send_sem.at[slot]

    def fem_peer(step):
        return (lax.rem(f + step + F, F), b)

    def flipped(flips):
        index = 0
        for i in range((F - 1).bit_length()):
            bit = lax.rem(f // (1 << i), 2)
            index += (1 - bit if flips >> i & 1 else bit) * (1 << i)
        return index

    def across_fem(flips):
        return (flipped(flips), b)

    def bem_peer(step):
        return (f, lax.rem(b + step + B, B))

    def remote(src, dst, place, ssem, rsem):
        return pltpu.make_async_remote_copy(
            src_ref=src,
            dst_ref=dst,
            send_sem=ssem,
            recv_sem=rsem,
            device_id=place,
            device_id_type=MESH,
        )

    def send(src, dst, place, key):
        copy = remote(src, dst, place, sender(key), recv_sem.at[next(arrivals)])
        copy.start()
        leaving[key] = copy.wait_send
        return copy.wait_recv

    def send_fem(src_of, dst_of, flips, size_ref, key):
        ssem, rsem = sender(key), recv_sem.at[next(arrivals)]
        for k in flips:
            remote(src_of(k), dst_of(k), across_fem(k), ssem, rsem).start()
        leaving[key] = pltpu.make_async_copy(size_ref, size_ref, ssem).wait
        return pltpu.make_async_copy(size_ref, size_ref, rsem).wait

    def fetch(src, dst):
        copy = pltpu.make_async_copy(src, dst, load_sem.at[next(loads)])
        copy.start()
        return copy

    opposite = F - 1
    nearby = range(1, F - 1)

    def spread(src_of, dst_ref, sign, key):
        ssem, rsem = sender(key), recv_sem.at[next(arrivals)]
        for s in range(1, B):
            remote(src_of(s), dst_ref.at[s], bem_peer(sign * s), ssem, rsem).start()
        rest = dst_ref.at[1:]
        leaving[key] = pltpu.make_async_copy(rest, rest, ssem).wait
        return pltpu.make_async_copy(rest, rest, rsem).wait

    whole_in = fetch(density_hbm, r.whole)
    small_in = [
        fetch(bank_hbm, r.bank),
        fetch(node_hbm, r.node),
        fetch(cell_hbm, r.cell),
    ]
    first = fetch(fem_hbm, r.fem[0].at[1 : d.cx + 1, 1 : d.cy + 1])
    right_in = fetch(right_hbm.at[pl.ds(b * pd, pd)], r.right)
    bsrc_in = fetch(bsrc_hbm.at[pl.ds(pl.multiple_of(f * share, share), share)], r.bsrc)
    load_in = fetch(load_hbm, r.load)
    other_in = [
        fetch(pairs_hbm, r.pairs),
        fetch(centers_hbm, r.centers),
        fetch(reaction_hbm, r.reaction),
        fetch(diag_hbm, r.diag),
        fetch(left_hbm, r.left),
        bsrc_in,
        load_in,
    ]

    barrier = pltpu.get_barrier_semaphore()
    for s in range(1, F):
        pl.semaphore_signal(barrier, inc=1, device_id=fem_peer(s), device_id_type=MESH)
    for s in range(1, B):
        pl.semaphore_signal(barrier, inc=1, device_id=bem_peer(s), device_id_type=MESH)
    blocks_in = [fetch(blocks_hbm.at[p], r.blocks.at[p]) for p in range(pd)]

    whole_in.wait()
    for p in range(pd):
        cols = slice(p * rows, (p + 1) * rows)
        r.x[0][home + p] = r.whole[:, cols].astype(BF16)
        r.den[p] = r.whole[pl.ds(pl.multiple_of(f * share, share), share), cols]
    pl.semaphore_wait(barrier, F - 1 + B - 1)

    def rows_of(index):
        return pl.ds(pl.multiple_of(index * share, share), share)

    own_rows, opposite_rows = rows_of(f), rows_of(flipped(opposite))
    state = Dims(
        faces={},
        fwd={},
        homes={},
        out={},
        own={},
        turned={},
        parts={},
        red={},
        sides={},
        val={},
        z={},
    )

    def partner_copy(n, p, which):
        x = r.x[n]
        if which == "home":
            there = jnp.where(odd == 0, -1, 1)
            source = home + p
        else:
            there = jnp.where(odd == 0, 1, -1)
            source = (REACH + 2 * there) * pd + p
        target = (REACH + there) * pd + p
        place = (f, b + 1 - 2 * odd)
        return send(x.at[pl.ds(source, 1)], x.at[pl.ds(target, 1)], place, (which, p))

    def along_bem(n, p, span, key):
        x = r.x[n]
        return {
            side: send(
                x.at[home + p, span],
                x.at[(REACH - side) * pd + p, span],
                bem_peer(side),
                (key, p, side),
            )
            for side in (2, -2)
        }

    def start_share(n, p):
        mine = r.x[n].at[home + p, own_rows]
        state.z[n, p] = along_bem(n, p, own_rows, "z")
        if n > 0:
            size = r.precv[n].at[p]
            state.own[n, p] = [
                send_fem(
                    lambda k: mine, lambda k: mine, flips, size.at[0 : len(flips)], (tag, p)
                )
                for tag, flips in (("far", (opposite,)), ("own", nearby))
            ]

    def turn(n, p):
        if n > 0:
            state.own[n, p][0]()
        state.turned[n, p] = along_bem(n, p, opposite_rows, "m")

    def forward(n, p):
        state.fwd[n, p] = []
        for side in (2, -2):
            state.z[n, p][side]()
            piece = r.x[n].at[(REACH - side) * pd + p, own_rows]
            size = r.precv[n].at[p, 0 : len(nearby)]
            state.fwd[n, p].append(
                send_fem(
                    lambda k: piece, lambda k: piece, nearby, size, ("fwd", p, side)
                )
            )

    def homes(n, p):
        if n > 0:
            state.own[n, p][1]()
        state.homes[n, p] = partner_copy(n, p, "home")

    def sides(n, p):
        for arrive in (*state.turned[n, p].values(), *state.fwd[n, p]):
            arrive()
        state.sides[n, p] = partner_copy(n, p, "sides")

    def reduce_own(n):
        total = 0.0
        for p in range(pd):
            mine = r.x[n][home + p, own_rows, :]
            total += dot(mine, r.right_wide[p], 1, 1)
        folded = (total[: share // 2] + pltpu.roll(total[share // 2 :], 64, 1)).astype(BF16)
        r.red_send[n][...] = folded
        r.red_recv[n][0] = folded
        state.red[n] = spread(lambda s: r.red_send[n], r.red_recv[n], 1, "red")

    def send_picked(n, acc):
        out = acc.astype(BF16).reshape(B, CAP, exc)
        r.out_send[n][...] = out
        r.out_recv[n][0] = out[0]
        state.out[n] = spread(lambda s: r.out_send[n].at[s], r.out_recv[n], 1, "out")

    def send_faces(n):
        fem = r.fem[n % 2]
        xs, ys = r.xface_send[n], r.yface_send[n]
        xr, yr = r.xface_recv[n], r.yface_recv[n]
        xs[0] = fem[d.cx, 1 : d.cy + 1].astype(BF16)
        xs[1] = fem[1, 1 : d.cy + 1].astype(BF16)
        ys[0] = fem[1 : d.cx + 1, d.cy].astype(BF16)
        ys[1] = fem[1 : d.cx + 1, 1].astype(BF16)
        waits = []
        for out, got, rank, size, peer in ((xs, xr, f, F, fem_peer), (ys, yr, b, B, bem_peer)):
            for i, step in enumerate((1, -1)):
                goes = rank < size - 1 if step == 1 else rank > 0
                comes = rank > 0 if step == 1 else rank < size - 1
                key = ("face", len(waits))
                copy = remote(out.at[i], got.at[i], peer(step), sender(key), recv_sem.at[next(arrivals)])
                pl.when(goes)(copy.start)
                leaving[key] = functools.partial(pl.when(goes), copy.wait_send)
                waits.append((comes, copy))
        state.faces[n] = waits

    def take_faces(n):
        fem = r.fem[n % 2]
        xr, yr = r.xface_recv[n], r.yface_recv[n]

        def put(i):
            if i == 0:
                fem[0, 1 : d.cy + 1] = xr[0].astype(F32)
            elif i == 1:
                fem[d.cx + 1, 1 : d.cy + 1] = xr[1].astype(F32)
            elif i == 2:
                fem[1 : d.cx + 1, 0] = yr[0].astype(F32)
            else:
                fem[1 : d.cx + 1, d.cy + 1] = yr[1].astype(F32)

        def clear(i):
            if i < 2:
                fem[(0, d.cx + 1)[i], 1 : d.cy + 1] = jnp.zeros((d.cy, d.cz, exc), F32)
            else:
                fem[1 : d.cx + 1, (0, d.cy + 1)[i - 2]] = jnp.zeros((d.cx, d.cz, exc), F32)

        for i, (comes, copy) in enumerate(state.faces[n]):

            def take(i=i, copy=copy):
                copy.wait_recv()
                put(i)

            pl.when(comes)(take)
            pl.when(jnp.logical_not(comes))(functools.partial(clear, i))

    def picked_first():
        def body(x, acc):
            plane = r.fem[0][x + 1, 1 : d.cy + 1].astype(BF16).reshape(d.cy * d.cz, exc)
            return acc + dot(r.pick_cell[x], plane)

        return lax.fori_loop(0, d.cx, body, jnp.zeros((d.dest, exc), F32))

    def fem_step(n):
        take_faces(n)
        state.val[n]()
        last = n == ITERS - 1
        old, fresh = r.fem[n % 2], r.fem[(n + 1) % 2]
        values = r.val_recv[n][...].reshape(d.dest, exc)
        level = lax.broadcasted_iota(jnp.int32, (d.cy, d.cz, exc), 1)

        def body(x, acc):
            coupled = dot(r.put_cell[x], values).reshape(d.cy, d.cz, exc)
            here = old[x + 1, 1 : d.cy + 1]
            beside = old[x, 1 : d.cy + 1] + old[x + 2, 1 : d.cy + 1]
            beside += old[x + 1, 0 : d.cy] + old[x + 1, 2 : d.cy + 2]
            beside += jnp.where(level > 0, pltpu.roll(here, 1, 1), 0.0)
            beside += jnp.where(level < d.cz - 1, pltpu.roll(here, d.cz - 1, 1), 0.0)
            result = (r.load[x] + beside - coupled) * r.inv[x]
            if last:
                fem_out[x] = result
                return acc
            fresh[x + 1, 1 : d.cy + 1] = result
            plane = result.astype(BF16).reshape(d.cy * d.cz, exc)
            return acc + dot(r.pick_cell[x], plane)

        acc = lax.fori_loop(0, d.cx, body, jnp.zeros((8 if last else d.dest, exc), F32))
        if not last:
            send_picked(n + 1, acc)

    def trace_values(n):
        values = 0.0
        for p in range(pd):
            values += dot(r.pick_row[:, p * rows : (p + 1) * rows], r.x[n][home + p], 1, 1)
        out = values.astype(BF16).reshape(B, CAP, exc)
        r.val_send[n][...] = out
        r.val_recv[n][0] = out[0]
        state.val[n] = spread(lambda s: r.val_send[n].at[s], r.val_recv[n], -1, "val")

    def trace_fem(n):
        state.out[n]()
        incoming = r.out_recv[n][...].reshape(d.dest, exc)
        r.traced[...] = dot(incoming, r.pick_row[...], 0, 0)

    def far(n):
        state.red[n]()
        for p in range(pd):
            total = jnp.zeros((share // 2, 128), F32)
            for s in range(B):
                scale = jnp.zeros((1, 128), F32)
                for q in range(pd):
                    at = lax.rem(b - s + B, B) * pd + q
                    group = (lane64 >= q * d.rank) & (lane64 < (q + 1) * d.rank)
                    scale = jnp.where(group, r.kernel[p, pl.ds(at, 1), :], scale)
                total += r.red_recv[n][s].astype(F32) * scale
            first = jnp.where(lane128 < 64, total, 0.0)
            second = jnp.where(lane128 < 64, pltpu.roll(total, 64, 1), 0.0)
            total = jnp.concatenate([first, second], axis=0)
            high = total.astype(BF16)
            low = (total - high.astype(F32)).astype(BF16)
            distant = dot(high, r.left_wide[p]) + dot(low, r.left_wide[p])
            cols = slice(p * rows, (p + 1) * rows)
            r.base[:, cols] = r.bsrc[:, cols] - distant

    def near(n):
        for p in range(pd):
            state.sides[n, p]()
            state.homes[n, p]()
        x = r.x[n]
        for p in range(pd):
            cols = slice(p * rows, (p + 1) * rows)
            acc = r.traced[:, cols]
            for k in range(d.group):
                pair = pairs_ref[p, f * d.group + k]
                spot = lax.rem(pair - b * pd + REACH * pd + B * pd, B * pd)
                spot = jnp.minimum(spot, (2 * REACH + 1) * pd - 1)
                acc += dot(x[spot], r.blocks[p, k])
            r.acc[p] = acc
            out, got = r.psend[n], r.precv[n]
            out[p] = acc.astype(BF16)
            state.parts[n, p] = send_fem(
                lambda k: out.at[p, rows_of(flipped(k))],
                lambda k: got.at[p, k - 1],
                range(F - 1, 0, -1),
                got.at[p],
                ("part", p),
            )

    def update(n, p):
        state.parts[n, p]()
        last = n == ITERS - 1
        cols = slice(p * rows, (p + 1) * rows)
        total = r.acc[p, own_rows, :]
        for k in range(F - 1):
            total += r.precv[n][p, k].astype(F32)
        fresh = r.den[p] + (r.base[:, cols] - total) / r.diag[:, cols]
        if last:
            bem_out[:, cols] = fresh
        else:
            r.den[p] = fresh
            r.x[n + 1][home + p, own_rows, :] = fresh.astype(BF16)
            start_share(n + 1, p)

    for p in range(pd):
        start_share(0, p)
    for p in range(pd):
        turn(0, p)
        homes(0, p)

    def column(row):
        size = row.shape[1]
        down = lax.broadcasted_iota(jnp.int32, (size, size), 0)
        across = lax.broadcasted_iota(jnp.int32, (size, size), 1)
        return jnp.sum(jnp.where(down == across, row, 0.0), axis=1, keepdims=True)

    count, dest = d.slots, d.dest
    lane128 = lax.broadcasted_iota(jnp.int32, (1, 128), 1)
    lane64 = lax.rem(lane128, 64)
    for copy in small_in:
        copy.wait()
    node_row = r.node[...].astype(F32)
    cell_row = r.cell[...].astype(F32)
    step_row = lax.rem(r.bank[...] - b + B, B).astype(F32)
    down = lax.broadcasted_iota(jnp.int32, (count, count), 0)
    across = lax.broadcasted_iota(jnp.int32, (count, count), 1)
    earlier = (column(step_row) == step_row) & (down < across)
    order = jnp.sum(jnp.where(earlier, 1.0, 0.0), axis=0, keepdims=True)
    target = step_row * CAP + order
    lands = lax.broadcasted_iota(jnp.int32, (dest, count), 0).astype(F32) == target
    cell_col = jnp.sum(jnp.where(lands, cell_row + 1.0, 0.0), axis=1, keepdims=True) - 1.0
    lands_t = lax.broadcasted_iota(jnp.int32, (count, dest), 1).astype(F32) == column(target)
    row_lane = (
        jnp.sum(jnp.where(lands_t, column(node_row) + 1.0, 0.0), axis=0, keepdims=True) - 1.0
    )
    r.row_send[...] = row_lane
    r.row_recv[0] = row_lane
    row_in = spread(lambda s: r.row_send, r.row_recv, 1, "row")

    for p in range(pd):
        forward(0, p)

    right_in.wait()
    for p in range(pd):
        r.right_wide[p] = jnp.zeros((128, rows), BF16)
        r.right_wide[p, p * d.rank : (p + 1) * d.rank, :] = r.right[p]
    reduce_own(0)

    plane = d.cy * d.cz
    ids_lane = lax.broadcasted_iota(jnp.int32, (dest, plane), 1).astype(F32)
    for x in range(d.cx):
        r.pick_cell[x] = hot(cell_col - float(x * plane) == ids_lane)
    first.wait()
    send_picked(0, picked_first())
    send_faces(0)

    def weights_setup():
        for copy in other_in:
            copy.wait()
        for p in range(pd):
            r.left_wide[p] = jnp.zeros((128, rows), BF16)
            for q in range(pd):
                r.left_wide[p, q * d.rank : (q + 1) * d.rank, :] = r.left[p]
        total = B * pd
        panel_row = lax.broadcasted_iota(jnp.int32, (1, total), 1)
        panel_col = lax.broadcasted_iota(jnp.int32, (total, 1), 0)
        for p in range(pd):
            own = b * pd + p
            square = jnp.zeros((total, 1), F32)
            for i in range(3):
                place = r.centers[i : i + 1, :]
                mine = jnp.sum(jnp.where(panel_row == own, place, 0.0), axis=1, keepdims=True)
                apart = mine - column(place)
                square += apart * apart
            named = jnp.where(r.pairs[p : p + 1, :] == panel_col, 1.0, 0.0)
            listed = jnp.max(named, axis=1, keepdims=True) + jnp.where(panel_col == own, 1.0, 0.0)
            weight = jnp.where(listed > 0.0, 0.0, 1.0 / (1.0 + square))
            r.kernel[p] = jnp.broadcast_to(weight, (total, 128))

    def finish_setup():
        cell_send = (
            jnp.sum(jnp.where(lands_t, column(cell_row) + 1.0, 0.0), axis=0, keepdims=True) - 1.0
        )
        ids_down = lax.broadcasted_iota(jnp.int32, (plane, dest), 0).astype(F32)
        for x in range(d.cx):
            r.put_cell[x] = hot(cell_send - float(x * plane) == ids_down)

        def spread_inverse(x, carry):
            inverse = 1.0 / (6.0 + r.reaction[x])
            for y in range(d.cy):
                wide = jnp.broadcast_to(column(inverse[y : y + 1, :]), (d.cz, exc))
                r.inv[x, y] = wide
            return carry

        lax.fori_loop(0, d.cx, spread_inverse, 0)

    for n in range(ITERS):
        last = n == ITERS - 1
        if n > 0:
            reduce_own(n)
            for p in range(pd):
                turn(n, p)
                forward(n, p)
            send_faces(n)
            for p in range(pd):
                homes(n, p)
        if n > 0:
            trace_values(n)
            far(n)
        if n == 0:
            for copy in blocks_in:
                copy.wait()
        for p in range(pd):
            sides(n, p)
        if n == 0:
            weights_setup()
            row_in()
            lanes = lax.broadcasted_iota(jnp.int32, (CAP, 128), 1).astype(F32)
            place_down = lax.broadcasted_iota(jnp.int32, (CAP, dest), 0)
            place_lane = lax.broadcasted_iota(jnp.int32, (CAP, dest), 1)
            for s in range(B):
                meant = place_lane == place_down + s * CAP
                wanted = jnp.sum(jnp.where(meant, r.row_recv[s], 0.0), axis=1, keepdims=True)
                for j in range(pd * rows // 128):
                    r.pick_row[s * CAP : (s + 1) * CAP, j * 128 : (j + 1) * 128] = hot(
                        wanted - float(j * 128) == lanes
                    )
            trace_values(n)
            far(n)
            finish_setup()
        trace_fem(n)
        near(n)
        fem_step(n)
        for p in range(pd):
            update(n, p)

    for finish in leaving.values():
        finish()


def hand_over(fem_in, bem_in, fem_out, bem_out, out_sem):
    moves = ((fem_in, fem_out), (bem_in, bem_out))
    outs = [pltpu.make_async_copy(m, o, out_sem.at[i]) for i, (m, o) in enumerate(moves)]
    for copy in outs:
        copy.start()
    for copy in outs:
        copy.wait()


class Dims:
    def __init__(self, **items):
        self.__dict__.update(items)


def shards(
    fem_field,
    fem_source,
    reaction,
    bem_density,
    bem_source,
    bem_diagonal,
    near_blocks,
    near_pairs,
    low_left,
    low_right,
    centers,
    trace_cell,
    trace_bank,
    trace_row,
):
    d = Dims()
    d.f, d.b = lax.axis_size("fem"), lax.axis_size("bem")
    d.pd, d.group, d.rows, _ = near_blocks.shape
    d.rank = low_right.shape[1]
    d.cx, d.cy, d.cz, d.exc = fem_field.shape
    d.share = d.exc // d.f
    d.slots = trace_cell.shape[0]
    d.dest = d.b * CAP
    d.pairs = near_pairs.shape[1]
    assert d.pd * d.rank <= 64

    items = jax.tree.leaves(layout(d))
    vmem = pl.BlockSpec(memory_space=pltpu.VMEM)
    far_off = pl.BlockSpec(memory_space=pltpu.HBM)
    results = pl.pallas_call(
        functools.partial(solve_kernel, d),
        out_shape=[
            pltpu.VMEM(fem_field.shape, F32),
            pltpu.VMEM((d.share, d.pd * d.rows), F32),
        ],
        in_specs=[pl.BlockSpec(memory_space=pltpu.SMEM)] + [far_off] * 14,
        out_specs=[vmem, vmem],
        scratch_shapes=items
        + [
            pltpu.SemaphoreType.DMA((30,)),
            pltpu.SemaphoreType.DMA((84,)),
            pltpu.SemaphoreType.DMA((17,)),
        ],
        cost_estimate=pl.CostEstimate(flops=1 << 33, bytes_accessed=1 << 24, transcendentals=0),
        compiler_params=pltpu.CompilerParams(
            collective_id=0, has_side_effects=True, vmem_limit_bytes=54 << 20
        ),
        name="sweeps",
    )(
        near_pairs,
        trace_bank.reshape(1, d.slots),
        trace_row[None, :],
        trace_cell[None, :],
        near_pairs,
        centers.T,
        reaction,
        bem_diagonal[None, :],
        low_left,
        fem_field,
        fem_source,
        bem_density,
        bem_source,
        near_blocks,
        low_right,
    )
    return pl.pallas_call(
        hand_over,
        out_shape=[jax.ShapeDtypeStruct(x.shape, x.dtype) for x in results],
        in_specs=[vmem] * 2,
        out_specs=[far_off] * 2,
        scratch_shapes=[pltpu.SemaphoreType.DMA((2,))],
        compiler_params=pltpu.CompilerParams(vmem_limit_bytes=4 << 20),
        name="hand_over",
    )(*results)


def solution(mesh):
    return jax.shard_map(
        shards,
        mesh=mesh,
        in_specs=(
            P("fem", "bem", None, None),
            P("fem", "bem", None, None),
            P("fem", "bem", None),
            P(None, "bem"),
            P(None, "bem"),
            P("bem"),
            P("bem", "fem", None, None),
            P("bem", None),
            P("bem", None, None),
            P(),
            P(),
            P(("fem", "bem")),
            P(("fem", "bem"), None),
            P(("fem", "bem")),
        ),
        out_specs=(P("fem", "bem", None, None), P("fem", "bem")),
        check_vma=False,
    )
```
